512 devices in a mesh: sweep: 2 (over y), row: 8 (over x, core), col: 32 (over z).
Axes of the slice: x: 4, y: 2, z: 32, core: 2. Of those that a mesh axis runs over, the one named last changes fastest.
The devices are a block of a 4x8x32 slice.
Arguments:
- tokens: bfloat16 [1280, 4096], P(('sweep', 'col'), 'row'), parts along dimension 0, may hold values from -6 to 6
- w_gate: bfloat16 [4096, 14336], P('row', 'col'), may hold values from -0.09375 to 0.09375
- w_up: bfloat16 [4096, 14336], P('row', 'col'), may hold values from -0.09375 to 0.09375
- w_down: bfloat16 [14336, 4096], P('col', 'row'), may hold values from -0.046875 to 0.046875
- cotangent: bfloat16 [1280, 4096], P(('sweep', 'col'), 'row'), parts along dimension 0, may hold values from -6 to 6
- step_rate: float32 [2], P('sweep'), parts along dimension 0, may hold values from 0.05 to 0.3
Outputs:
- out_rows: bfloat16 [1280, 4096], P(('sweep', 'col'), 'row'), parts along dimension 0
- grad_in: bfloat16 [1280, 4096], P(('sweep', 'col'), 'row'), parts along dimension 0
- step_gate: bfloat16 [8192, 14336], P(('sweep', 'row'), 'col'), parts along dimension 0
- step_up: bfloat16 [8192, 14336], P(('sweep', 'row'), 'col'), parts along dimension 0
- step_down: bfloat16 [28672, 4096], P(('sweep', 'col'), 'row'), parts along dimension 0
The draws below stay inside these ranges and needn't reach their ends.
There are 2 independent parts, one for each index of `sweep`. The reference program is written for one: setup_inputs(seed, part) draws one part's arguments, and reference() takes and returns one part's arrays. A program takes and returns all parts, laid end to end along the dimension named above; an argument that names none is the same for every part. Nothing has to cross between parts.
All inputs are finite; a program needn't handle non-finite values.
Results may differ from the reference program's by a relative error of at most 0.0049.
Values may be sent and summed in bfloat16 or wider, within the bound.
No kernel may reach another device: no remote copies, remote signals or barrier semaphores. Data moves between devices by JAX's collectives and lax.ppermute only.
A program may use at most 64 MiB of HBM per device.

```python
import math
import jax
import jax.numpy as jnp

D = 4096
FF = 14336
TOKENS = 640


def levels(stream_key, shape, shards, low, high):
    gain = 1.0
    for dim, parts in shards:
        steps = jax.random.uniform(jax.random.fold_in(jax.random.fold_in(stream_key, 6), dim), (parts,), jnp.float32, low / len(shards), high / len(shards))
        gain = gain * jnp.repeat(jnp.exp(steps), shape[dim] // parts).reshape((-1,) + (1,) * (len(shape) - 1 - dim))
    return gain


def noise(stream_key, dims, deviation, limit, cuts=(), held_as=jnp.bfloat16):
    values = jax.random.normal(stream_key, dims, jnp.float32) * deviation
    if len(cuts) > 0:
        values = levels(stream_key, dims, cuts, -0.22, 0.18) * values
    return jnp.clip(values, min=-limit, max=limit).astype(held_as)


def setup_inputs(seed: int = 0, part: int = 0) -> dict:
    seeds = jax.random.split(jax.random.key(seed), 7)
    part_keys = jax.random.split(jax.random.fold_in(seeds[6], part), 7)
    return {
        "tokens": noise(part_keys[0], (TOKENS, D), 1.0, 6.0, ((0, 32), (1, 8))),
        "w_gate": noise(seeds[1], (D, FF), D ** -0.5, 0.09375, ((0, 8), (1, 32))),
        "w_up": noise(seeds[2], (D, FF), D ** -0.5, 0.09375, ((0, 8), (1, 32))),
        "w_down": noise(seeds[3], (FF, D), FF ** -0.5, 0.046875, ((0, 32), (1, 8))),
        "cotangent": noise(part_keys[4], (TOKENS, D), 1.0, 6.0, ((0, 32), (1, 8))),
        "step_rate": jnp.clip(jnp.exp(jax.random.uniform(part_keys[5], (1,), jnp.float32, math.log(0.05), math.log(0.3))), 0.05, 0.3),
    }


def reference(tokens, w_gate, w_up, w_down, cotangent, step_rate):
    gate_val = jnp.dot(tokens, w_gate, preferred_element_type=jnp.float32)
    up_val = jnp.dot(tokens, w_up, preferred_element_type=jnp.float32)
    gate_sig = jax.nn.sigmoid(gate_val)
    activation = gate_val * gate_sig
    hidden = (activation * up_val).astype(jnp.bfloat16)
    out_rows = (tokens.astype(jnp.float32) + jnp.dot(hidden, w_down, preferred_element_type=jnp.float32)).astype(jnp.bfloat16)
    back_hidden = jnp.dot(cotangent, w_down.T, preferred_element_type=jnp.float32)
    back_gate = (back_hidden * up_val * gate_sig * (1.0 + gate_val * (1.0 - gate_sig))).astype(jnp.bfloat16)
    back_up = (back_hidden * activation).astype(jnp.bfloat16)
    grad_total = cotangent.astype(jnp.float32) + jnp.dot(back_gate, w_gate.T, preferred_element_type=jnp.float32)
    grad_in = (grad_total + jnp.dot(back_up, w_up.T, preferred_element_type=jnp.float32)).astype(jnp.bfloat16)
    factor = -step_rate[0]
    step_gate = (factor * jnp.dot(tokens.T, back_gate, preferred_element_type=jnp.float32)).astype(jnp.bfloat16)
    step_up = (factor * jnp.dot(tokens.T, back_up, preferred_element_type=jnp.float32)).astype(jnp.bfloat16)
    step_down = (factor * jnp.dot(hidden.T, cotangent, preferred_element_type=jnp.float32)).astype(jnp.bfloat16)
    return out_rows, grad_in, step_gate, step_up, step_down
```

```python
import jax
import jax.numpy as jnp
from jax import lax
from jax.experimental.layout import Layout, with_layout_constraint
from jax.sharding import PartitionSpec as P

BF16 = jnp.bfloat16
F32 = jnp.float32
NT = (((1,), (1,)), ((), ()))
NN = (((1,), (0,)), ((), ()))
TN = (((0,), (0,)), ((), ()))


def dot(left, right, dims):
    return lax.dot_general(left, right, dims, preferred_element_type=F32)


def row_major(value):
    return with_layout_constraint(value, Layout(major_to_minor=tuple(range(value.ndim))))


def round_up(value, unit):
    return -(-value // unit) * unit


def col_shift(value, step):
    size = lax.axis_size("col")
    return lax.ppermute(value, "col", [(i, (i + step) % size) for i in range(size)])


def parity_groups():
    size = lax.axis_size("col")
    return [list(range(first, size, 2)) for first in range(2)]


def gather_col(block):
    own = lax.all_gather(block, "col", axis=0, tiled=True, axis_index_groups=parity_groups())
    half = own.shape[0] // 2
    low = col_shift(own[:half], 1)
    high = col_shift(own[half:], -1)
    return jnp.concatenate([own, low, high], axis=0)


def scatter_col(parts):
    size = lax.axis_size("col")
    members = size // 2
    rows = parts.shape[0] // size
    width = parts.shape[1]
    count = parts.shape[0] // 2
    half = count // 2
    other = parts[count:].astype(BF16)
    low = col_shift(other[:half], -1)
    high = col_shift(other[half:], 1)
    mine = parts[:count] + jnp.concatenate([low, high], axis=0).astype(F32)
    padded = round_up(rows + 1, 8) - 1
    mine = mine.reshape(members, rows, width)
    mine = jnp.pad(mine, ((0, 0), (0, padded - rows), (0, 0))).reshape(members * padded, width)
    summed = lax.psum_scatter(
        mine, "col", scatter_dimension=0, tiled=True, axis_index_groups=parity_groups()
    )
    return lax.optimization_barrier(summed)[:rows]


def local(tokens, w_gate, w_up, w_down, cotangent, step_rate):
    features = tokens.shape[1]
    hidden_width = w_gate.shape[1]
    n_row = lax.axis_size("row")
    share = hidden_width // n_row
    both = gather_col(jnp.concatenate([tokens, cotangent], axis=1))
    tokens_all = both[:, :features]
    cotangent_all = both[:, features:]
    n_tokens = both.shape[0]

    gate_part = dot(w_gate.T, tokens_all, NT).astype(BF16)
    up_part = dot(w_up.T, tokens_all, NT).astype(BF16)
    back_part = dot(w_down, cotangent_all, NT).astype(BF16)
    parts = jnp.stack(
        [v.reshape(n_row, share, n_tokens) for v in (gate_part, up_part, back_part)], axis=1
    )
    arrived = lax.all_to_all(parts, "row", 0, 0, tiled=True)
    summed = jnp.sum(arrived.astype(F32), axis=0)
    gate_val, up_val, back_hidden = summed[0], summed[1], summed[2]
    gate_sig = jax.nn.sigmoid(gate_val)
    activation = gate_val * gate_sig
    hidden = (activation * up_val).astype(BF16)
    back_gate = (back_hidden * up_val * gate_sig * (1.0 + gate_val * (1.0 - gate_sig))).astype(BF16)
    back_up = (back_hidden * activation).astype(BF16)
    mine = jnp.stack([hidden, back_gate, back_up])
    full = lax.all_to_all(
        jnp.broadcast_to(mine[None], (n_row, *mine.shape)), "row", 0, 0, tiled=True
    )
    hidden_all, gate_grad_all, up_grad_all = (
        full[:, k].reshape(hidden_width, n_tokens) for k in range(3)
    )

    out_part = dot(hidden_all, w_down, TN)
    grad_part = dot(gate_grad_all, w_gate.T, TN) + dot(up_grad_all, w_up.T, TN)
    sums = scatter_col(row_major(jnp.concatenate([out_part, grad_part], axis=1)))
    out_rows = (tokens.astype(F32) + sums[:, :features]).astype(BF16)
    grad_in = (cotangent.astype(F32) + sums[:, features:]).astype(BF16)

    factor = -step_rate[0]
    step_gate = (factor * dot(gate_grad_all, tokens_all, NN)).astype(BF16).T
    step_up = (factor * dot(up_grad_all, tokens_all, NN)).astype(BF16).T
    step_down = (factor * dot(hidden_all, cotangent_all, NN)).astype(BF16)
    return (out_rows, grad_in, step_gate, step_up, step_down)


def solution(mesh):
    in_specs = (
        P(("sweep", "col"), "row"),
        P("row", "col"),
        P("row", "col"),
        P("col", "row"),
        P(("sweep", "col"), "row"),
        P("sweep"),
    )
    out_specs = (
        P(("sweep", "col"), "row"),
        P(("sweep", "col"), "row"),
        P(("sweep", "row"), "col"),
        P(("sweep", "row"), "col"),
        P(("sweep", "col"), "row"),
    )
    return jax.shard_map(local, mesh=mesh, in_specs=in_specs, out_specs=out_specs, check_vma=False)
```

```python
import jax
import jax.numpy as jnp
from jax import lax
from jax.experimental.layout import Layout, with_layout_constraint
from jax.sharding import PartitionSpec as P


BF16 = jnp.bfloat16
F32 = jnp.float32
LANES = 128
NT = (((1,), (1,)), ((), ()))
NN = (((1,), (0,)), ((), ()))
TN = (((0,), (0,)), ((), ()))


def dot(left, right, dims):
    return lax.dot_general(left, right, dims, preferred_element_type=F32)


def row_major(value):
    return with_layout_constraint(value, Layout(major_to_minor=tuple(range(value.ndim))))


def round_up(value, unit):
    return -(-value // unit) * unit


def col_shift(value, step):
    size = lax.axis_size("col")
    return lax.ppermute(value, "col", [(i, (i + step) % size) for i in range(size)])


def every_other(axis):
    size = lax.axis_size(axis)
    return [list(range(first, size, 2)) for first in range(2)]


def scatter_col(parts):
    members = lax.axis_size("col") // 2
    rows = parts.shape[0] // members
    width = parts.shape[1]
    padded = round_up(rows + 1, 8) - 1
    parts = parts.reshape(members, rows, width)
    parts = jnp.pad(parts, ((0, 0), (0, padded - rows), (0, 0)))
    parts = parts.reshape(members * padded, width)
    summed = lax.psum_scatter(
        parts, "col", scatter_dimension=0, tiled=True, axis_index_groups=every_other("col")
    )
    return lax.optimization_barrier(summed)[:rows]


def gather_row(block):
    size = lax.axis_size("row")
    mine = lax.all_gather(block, "row", axis=0, axis_index_groups=every_other("row"))
    pair = lax.ppermute(mine, "row", [(i, i ^ 1) for i in range(size)])
    even = lax.axis_index("row") % 2 == 0
    full = jnp.stack([jnp.where(even, mine, pair), jnp.where(even, pair, mine)], axis=1)
    return full.reshape(size * block.shape[0], block.shape[1])


def layer(tokens, w_gate, w_up, w_down, cotangent, step_rate):
    features = tokens.shape[1]
    own = w_gate.shape[1]
    n_row = lax.axis_size("row")
    low = round_up(own // 2, LANES)
    high = own - low
    width = 2 * own
    window = own // LANES * LANES
    extra = own - window

    weights = jnp.stack([w_gate.T, w_up.T, w_down])
    from_below = col_shift(weights[:, low:], 1)
    from_above = col_shift(weights[:, :low], -1)
    block = jnp.concatenate([tokens, cotangent], axis=1)
    both = lax.all_gather(block, "col", axis=0, tiled=True, axis_index_groups=every_other("col"))
    count = both.shape[0]
    half = count // 2
    other = jnp.concatenate(
        [col_shift(both[:half], 1), col_shift(both[half:], -1)],
        axis=0,
    )
    w_gate_t, w_up_t, w_down_t = (
        jnp.concatenate([weights[k], from_below[k], from_above[k]], axis=0) for k in range(3)
    )
    tokens_own, cotangent_own = both[:, :features], both[:, features:]
    tokens_other, cotangent_other = other[:, :features], other[:, features:]

    parts = [
        dot(tokens_own, w_gate_t, NT).astype(BF16),
        dot(tokens_own, w_up_t, NT).astype(BF16),
        dot(cotangent_own, w_down_t, NT).astype(BF16),
    ]
    parts = jnp.concatenate(parts, axis=1)
    parts = parts.reshape(n_row, count // n_row, 3 * width)
    arrived = lax.all_to_all(parts, "row", 0, 0, tiled=True)
    summed = jnp.sum(arrived.astype(F32), axis=0)
    gate_val, up_val, back_hidden = (summed[:, k * width : (k + 1) * width] for k in range(3))
    gate_sig = jax.nn.sigmoid(gate_val)
    activation = gate_val * gate_sig
    hidden = (activation * up_val).astype(BF16)
    back_gate = (back_hidden * up_val * gate_sig * (1.0 + gate_val * (1.0 - gate_sig))).astype(BF16)
    back_up = (back_hidden * activation).astype(BF16)
    full = gather_row(jnp.concatenate([hidden, back_gate, back_up], axis=1))
    parts_of = [full[:, k * width : (k + 1) * width] for k in range(3)]

    to_below = jnp.stack([v[:, window : own + high] for v in parts_of])
    to_above = jnp.stack([v[:, own + high :] for v in parts_of])
    high_other = col_shift(to_below, -1)
    low_other = col_shift(to_above, 1)

    out_part = dot(parts_of[0], w_down_t, NN)
    grad_part = dot(parts_of[1], w_gate_t, NN) + dot(parts_of[2], w_up_t, NN)
    sums = scatter_col(row_major(jnp.concatenate([out_part, grad_part], axis=1)))
    out_rows = (tokens.astype(F32) + sums[:, :features]).astype(BF16)
    grad_in = (cotangent.astype(F32) + sums[:, features:]).astype(BF16)

    factor = -step_rate[0]

    def step(k, rows_own, rows_other):
        mine = dot(parts_of[k][:, :own], rows_own, TN)
        upper = dot(high_other[k], rows_other, TN)[extra:]
        lower = dot(low_other[k], rows_other, TN)
        return (factor * (mine + jnp.concatenate([lower, upper], axis=0))).astype(BF16)

    step_down = step(0, cotangent_own, cotangent_other)
    step_gate = step(1, tokens_own, tokens_other).T
    step_up = step(2, tokens_own, tokens_other).T
    return (out_rows, grad_in, step_gate, step_up, step_down)


def solution(mesh):
    in_specs = (
        P(("sweep", "col"), "row"),
        P("row", "col"),
        P("row", "col"),
        P("col", "row"),
        P(("sweep", "col"), "row"),
        P("sweep"),
    )
    out_specs = (
        P(("sweep", "col"), "row"),
        P(("sweep", "col"), "row"),
        P(("sweep", "row"), "col"),
        P(("sweep", "row"), "col"),
        P(("sweep", "col"), "row"),
    )
    return jax.shard_map(layer, mesh=mesh, in_specs=in_specs, out_specs=out_specs, check_vma=False)
```

```python
import jax
import jax.numpy as jnp
from jax import lax
from jax.experimental.layout import Layout, with_layout_constraint
from jax.sharding import PartitionSpec as P

BF16 = jnp.bfloat16
F32 = jnp.float32
NT = (((1,), (1,)), ((), ()))
NN = (((1,), (0,)), ((), ()))
TN = (((0,), (0,)), ((), ()))


def dot(left, right, dims):
    return lax.dot_general(left, right, dims, preferred_element_type=F32)


def row_major(value):
    return with_layout_constraint(value, Layout(major_to_minor=tuple(range(value.ndim))))


def round_up(value, unit):
    return -(-value // unit) * unit


def every_other(axis):
    size = lax.axis_size(axis)
    return [list(range(first, size, 2)) for first in range(2)]


def move(value, swap, step):
    rows, cols = lax.axis_size("row"), lax.axis_size("col")
    pairs = []
    for row in range(rows):
        for col in range(cols):
            to_row = row ^ 1 if swap else row
            to_col = (col + (step if row % 2 == 0 else -step)) % cols
            pairs.append((row * cols + col, to_row * cols + to_col))
    return lax.ppermute(value, ("row", "col"), pairs)


def gather_col(block):
    return lax.all_gather(block, "col", axis=0, tiled=True, axis_index_groups=every_other("col"))


def scatter_col(parts):
    members = lax.axis_size("col") // 2
    rows = parts.shape[0] // members
    width = parts.shape[1]
    padded = round_up(rows + 1, 8) - 1
    parts = parts.reshape(members, rows, width)
    parts = jnp.pad(parts, ((0, 0), (0, padded - rows), (0, 0))).reshape(members * padded, width)
    summed = lax.psum_scatter(
        parts, "col", scatter_dimension=0, tiled=True, axis_index_groups=every_other("col")
    )
    return lax.optimization_barrier(summed)[:rows]


def layer(tokens, w_gate, w_up, w_down, cotangent, step_rate):
    features = tokens.shape[1]
    own = w_gate.shape[1]
    core = lax.axis_index("row") % 2
    first = core == 0
    weights = jnp.concatenate([w_gate.T, w_up.T, w_down], axis=0)

    gathered = gather_col(jnp.concatenate([tokens, cotangent], axis=1))
    count = gathered.shape[0]
    half = count // 2
    same = lax.dynamic_slice_in_dim(gathered, core * half, half)
    cross = lax.dynamic_slice_in_dim(gathered, (1 - core) * half, half)
    rows_own = jnp.concatenate([same, move(same, False, 1)], axis=0)
    rows_pair = jnp.concatenate([move(cross, True, 0), move(cross, True, -1)], axis=0)
    weights_pair = move(weights, True, 0)

    wide = 2 * own
    tall = 3 * own
    both_part = dot(rows_own[:, :features], weights[:wide], NT) + dot(
        rows_pair[:, :features], weights_pair[:wide], NT
    )
    back_part = dot(rows_own[:, features:], weights[wide:], NT) + dot(
        rows_pair[:, features:], weights_pair[wide:], NT
    )
    parts = jnp.concatenate([both_part.astype(BF16), back_part.astype(BF16)], axis=1)
    members = lax.axis_size("row") // 2
    arrived = lax.all_to_all(
        parts.reshape(members, count // members, tall),
        "row",
        0,
        0,
        axis_index_groups=every_other("row"),
        tiled=True,
    )
    summed = jnp.sum(arrived.astype(F32), axis=0)
    gate_val, up_val, back_hidden = (summed[:, k * own : (k + 1) * own] for k in range(3))
    gate_sig = jax.nn.sigmoid(gate_val)
    activation = gate_val * gate_sig
    hidden = (activation * up_val).astype(BF16)
    back_gate = (back_hidden * up_val * gate_sig * (1.0 + gate_val * (1.0 - gate_sig))).astype(BF16)
    back_up = (back_hidden * activation).astype(BF16)
    acts = lax.all_gather(
        jnp.concatenate([back_gate, back_up, hidden], axis=1),
        "row",
        axis=0,
        tiled=True,
        axis_index_groups=every_other("row"),
    )

    def outputs(matrix):
        return row_major(
            jnp.concatenate(
                [dot(acts[:, wide:], matrix[wide:], NN), dot(acts[:, :wide], matrix[:wide], NN)],
                axis=1,
            )
        )

    out_pair = outputs(weights_pair).astype(BF16)
    out_own = outputs(weights)
    far = move(out_pair[half:], True, -1)
    near = move(out_own[half:].astype(BF16), False, -1)
    pair = move(out_pair[:half], True, 0)
    sum_same = out_own[:half] + near.astype(F32)
    sum_cross = pair.astype(F32) + far.astype(F32)
    sums = scatter_col(
        jnp.concatenate(
            [jnp.where(first, sum_same, sum_cross), jnp.where(first, sum_cross, sum_same)], axis=0
        )
    )
    out_rows = (tokens.astype(F32) + sums[:, :features]).astype(BF16)
    grad_in = (cotangent.astype(F32) + sums[:, features:]).astype(BF16)

    acts_pair = move(acts, True, 0)
    rows_rest = move(rows_pair, True, 0)
    factor = -step_rate[0]
    steps_in = dot(acts[:, :wide], rows_own[:, :features], TN) + dot(
        acts_pair[:, :wide], rows_rest[:, :features], TN
    )
    steps_out = dot(acts[:, wide:], rows_own[:, features:], TN) + dot(
        acts_pair[:, wide:], rows_rest[:, features:], TN
    )
    steps_in = (factor * steps_in).astype(BF16)
    step_down = (factor * steps_out).astype(BF16)
    return (out_rows, grad_in, steps_in[:own].T, steps_in[own:].T, step_down)


def solution(mesh):
    in_specs = (
        P(("sweep", "col"), "row"),
        P("row", "col"),
        P("row", "col"),
        P("col", "row"),
        P(("sweep", "col"), "row"),
        P("sweep"),
    )
    out_specs = (
        P(("sweep", "col"), "row"),
        P(("sweep", "col"), "row"),
        P(("sweep", "row"), "col"),
        P(("sweep", "row"), "col"),
        P(("sweep", "col"), "row"),
    )
    return jax.shard_map(layer, mesh=mesh, in_specs=in_specs, out_specs=out_specs, check_vma=False)
```

```python
import jax
import jax.numpy as jnp
from jax import lax
from jax.experimental.layout import Layout, with_layout_constraint
from jax.sharding import PartitionSpec as P


BF16 = jnp.bfloat16
F32 = jnp.float32
NT = (((1,), (1,)), ((), ()))
NN = (((1,), (0,)), ((), ()))
TN = (((0,), (0,)), ((), ()))


def dot(left, right, dims):
    return lax.dot_general(left, right, dims, preferred_element_type=F32)


def row_major(value):
    return with_layout_constraint(value, Layout(major_to_minor=tuple(range(value.ndim))))


def round_up(value, unit):
    return -(-value // unit) * unit


def every_other(axis):
    size = lax.axis_size(axis)
    return [list(range(first, size, 2)) for first in range(2)]


def move(value, swap, step):
    rows, cols = lax.axis_size("row"), lax.axis_size("col")
    pairs = []
    for row in range(rows):
        for col in range(cols):
            to_row = row ^ 1 if swap else row
            to_col = (col + (step if row % 2 == 0 else -step)) % cols
            pairs.append((row * cols + col, to_row * cols + to_col))
    return lax.ppermute(value, ("row", "col"), pairs)


def gather_col(block):
    return lax.all_gather(block, "col", axis=0, tiled=True, axis_index_groups=every_other("col"))


def scatter_col(parts):
    members = lax.axis_size("col") // 2
    rows = parts.shape[0] // members
    width = parts.shape[1]
    padded = round_up(rows + 1, 8) - 1
    parts = parts.reshape(members, rows, width)
    parts = jnp.pad(parts, ((0, 0), (0, padded - rows), (0, 0))).reshape(members * padded, width)
    summed = lax.psum_scatter(
        parts, "col", scatter_dimension=0, tiled=True, axis_index_groups=every_other("col")
    )
    return lax.optimization_barrier(summed)[:rows]


def layer(tokens, w_gate, w_up, w_down, cotangent, step_rate):
    features = tokens.shape[1]
    own = w_gate.shape[1]
    core = lax.axis_index("row") % 2
    first = core == 0
    gathered = gather_col(jnp.concatenate([tokens, cotangent], axis=1))
    count = gathered.shape[0]
    half = count // 2
    same = lax.dynamic_slice_in_dim(gathered, core * half, half)
    cross = lax.dynamic_slice_in_dim(gathered, (1 - core) * half, half)
    same, cross, w_gate, w_up, w_down = lax.optimization_barrier(
        (same, cross, w_gate, w_up, w_down)
    )
    weights = jnp.concatenate([w_gate.T, w_up.T, w_down], axis=0)
    rows_own = jnp.concatenate([same, move(same, False, 1)], axis=0)
    rows_pair = jnp.concatenate([move(cross, True, 0), move(cross, True, -1)], axis=0)
    weights_pair = move(weights, True, 0)

    wide = 2 * own
    tall = 3 * own
    both_part = dot(rows_own[:, :features], weights[:wide], NT) + dot(
        rows_pair[:, :features], weights_pair[:wide], NT
    )
    back_part = dot(rows_own[:, features:], weights[wide:], NT) + dot(
        rows_pair[:, features:], weights_pair[wide:], NT
    )
    parts = jnp.concatenate([both_part.astype(BF16), back_part.astype(BF16)], axis=1)
    members = lax.axis_size("row") // 2
    arrived = lax.all_to_all(
        parts.reshape(members, count // members, tall),
        "row",
        0,
        0,
        axis_index_groups=every_other("row"),
        tiled=True,
    )
    summed = jnp.sum(arrived.astype(F32), axis=0)
    gate_val, up_val, back_hidden = (summed[:, k * own : (k + 1) * own] for k in range(3))
    gate_sig = jax.nn.sigmoid(gate_val)
    activation = gate_val * gate_sig
    hidden = (activation * up_val).astype(BF16)
    back_gate = (back_hidden * up_val * gate_sig * (1.0 + gate_val * (1.0 - gate_sig))).astype(BF16)
    back_up = (back_hidden * activation).astype(BF16)
    acts = lax.all_gather(
        jnp.concatenate([back_gate, back_up, hidden], axis=1),
        "row",
        axis=0,
        tiled=True,
        axis_index_groups=every_other("row"),
    )

    def outputs(matrix):
        return row_major(
            jnp.concatenate(
                [dot(acts[:, wide:], matrix[wide:], NN), dot(acts[:, :wide], matrix[:wide], NN)],
                axis=1,
            )
        )

    out_pair = outputs(weights_pair).astype(BF16)
    out_own = outputs(weights)
    far, near, pair = out_pair[half:], out_own[half:].astype(BF16), out_pair[:half]
    far, near, pair, held = lax.optimization_barrier((far, near, pair, acts))
    far = move(far, True, -1)
    near = move(near, False, -1)
    pair = move(pair, True, 0)

    def partial_steps(rows):
        return [
            dot(held[:, :wide], rows[:, :features], TN),
            dot(held[:, wide:], rows[:, features:], TN),
        ]

    steps_rest = [value.astype(BF16) for value in partial_steps(rows_pair)]
    steps_rest = move(jnp.concatenate(steps_rest, axis=0), True, 0)
    in_own, out_own_steps = lax.optimization_barrier(partial_steps(rows_own))

    sum_same = out_own[:half] + near.astype(F32)
    sum_cross = pair.astype(F32) + far.astype(F32)
    sums = scatter_col(
        jnp.concatenate(
            [jnp.where(first, sum_same, sum_cross), jnp.where(first, sum_cross, sum_same)], axis=0
        )
    )
    factor = -step_rate[0]

    def step(mine, rest):
        return (factor * (mine + rest.astype(F32))).astype(BF16)

    sums, step_gate, step_up, step_down = lax.optimization_barrier(
        (
            sums,
            step(in_own[:own], steps_rest[:own]),
            step(in_own[own:], steps_rest[own:wide]),
            step(out_own_steps, steps_rest[wide:]),
        )
    )
    out_rows = (tokens.astype(F32) + sums[:, :features]).astype(BF16)
    grad_in = (cotangent.astype(F32) + sums[:, features:]).astype(BF16)
    return (out_rows, grad_in, step_gate.T, step_up.T, step_down)


def solution(mesh):
    in_specs = (
        P(("sweep", "col"), "row"),
        P("row", "col"),
        P("row", "col"),
        P("col", "row"),
        P(("sweep", "col"), "row"),
        P("sweep"),
    )
    out_specs = (
        P(("sweep", "col"), "row"),
        P(("sweep", "col"), "row"),
        P(("sweep", "row"), "col"),
        P(("sweep", "row"), "col"),
        P(("sweep", "col"), "row"),
    )
    return jax.shard_map(layer, mesh=mesh, in_specs=in_specs, out_specs=out_specs, check_vma=False)
```

```python
import jax
import jax.numpy as jnp
from jax import lax
from jax.experimental import pallas as pl
from jax.experimental.layout import Layout, with_layout_constraint
from jax.experimental.pallas import tpu as pltpu
from jax.sharding import PartitionSpec as P


BF16 = jnp.bfloat16
F32 = jnp.float32
NT = (((1,), (1,)), ((), ()))
NN = (((1,), (0,)), ((), ()))
TN = (((0,), (0,)), ((), ()))


def dot(left, right, dims):
    return lax.dot_general(left, right, dims, preferred_element_type=F32)


def row_major(value):
    return with_layout_constraint(value, Layout(major_to_minor=tuple(range(value.ndim))))


def round_up(value, unit):
    return -(-value // unit) * unit


def every_other(axis):
    size = lax.axis_size(axis)
    return [list(range(first, size, 2)) for first in range(2)]


def move(value, swap, step):
    rows, cols = lax.axis_size("row"), lax.axis_size("col")
    pairs = []
    for row in range(rows):
        for col in range(cols):
            to_row = row ^ 1 if swap else row
            to_col = (col + (step if row % 2 == 0 else -step)) % cols
            pairs.append((row * cols + col, to_row * cols + to_col))
    return lax.ppermute(value, ("row", "col"), pairs)


def gather_col(block):
    return lax.all_gather(block, "col", axis=0, tiled=True, axis_index_groups=every_other("col"))


def spread(core, out_own, grad_own, near, pair, far, rows, padded):
    half, width = near.shape
    features = out_own.shape[1]
    blocks = half // rows

    def kernel(core_ref, out_ref, grad_ref, near_ref, pair_ref, far_ref, sums_ref, same_ref, cross_ref):
        near_rows = near_ref[...].astype(F32)
        same_ref[:, :features] = out_ref[...] + near_rows[:, :features]
        same_ref[:, features:] = grad_ref[...] + near_rows[:, features:]
        cross_ref[...] = pair_ref[...].astype(F32) + far_ref[...].astype(F32)
        for block in range(2 * blocks):
            gap = padded - rows
            sums_ref[block * padded + rows : (block + 1) * padded, :] = jnp.zeros((gap, width), F32)

        def write(low, high):
            for block in range(blocks):
                source = slice(block * rows, (block + 1) * rows)
                for offset, part in ((0, low), (blocks, high)):
                    start = (offset + block) * padded
                    sums_ref[start : start + rows, :] = part[source, :]

        @pl.when(core_ref[0] == 0)
        def _():
            write(same_ref, cross_ref)

        @pl.when(core_ref[0] != 0)
        def _():
            write(cross_ref, same_ref)

    whole = pl.BlockSpec((half, width), lambda _: (0, 0))
    upper = pl.BlockSpec((half, features), lambda _: (0, 0))
    return pl.pallas_call(
        kernel,
        grid=(1,),
        out_shape=jax.ShapeDtypeStruct((2 * blocks * padded, width), F32),
        in_specs=[pl.BlockSpec(memory_space=pltpu.SMEM), upper, upper, whole, whole, whole],
        out_specs=pl.BlockSpec((2 * blocks * padded, width), lambda _: (0, 0)),
        scratch_shapes=[pltpu.VMEM((half, width), F32), pltpu.VMEM((half, width), F32)],
        compiler_params=pltpu.CompilerParams(vmem_limit_bytes=16 << 20),
        name="spread",
    )(core[None], out_own, grad_own, near, pair, far)


def scatter_col(parts, rows):
    summed = lax.psum_scatter(
        parts, "col", scatter_dimension=0, tiled=True, axis_index_groups=every_other("col")
    )
    return lax.optimization_barrier(summed)[:rows]


def layer(tokens, w_gate, w_up, w_down, cotangent, step_rate):
    features = tokens.shape[1]
    own = w_gate.shape[1]
    core = lax.axis_index("row") % 2
    gathered = gather_col(jnp.concatenate([tokens, cotangent], axis=1))
    count = gathered.shape[0]
    half = count // 2
    same = lax.dynamic_slice_in_dim(gathered, core * half, half)
    cross = lax.dynamic_slice_in_dim(gathered, (1 - core) * half, half)
    same, cross, w_gate, w_up, w_down = lax.optimization_barrier(
        (same, cross, w_gate, w_up, w_down)
    )
    weights = jnp.concatenate([w_gate.T, w_up.T, w_down], axis=0)
    rows_own = jnp.concatenate([same, move(same, False, 1)], axis=0)
    rows_pair = jnp.concatenate([move(cross, True, 0), move(cross, True, -1)], axis=0)
    weights_pair = move(weights, True, 0)

    wide = 2 * own
    tall = 3 * own
    both_part = dot(rows_own[:, :features], weights[:wide], NT) + dot(
        rows_pair[:, :features], weights_pair[:wide], NT
    )
    back_part = dot(rows_own[:, features:], weights[wide:], NT) + dot(
        rows_pair[:, features:], weights_pair[wide:], NT
    )
    parts = jnp.concatenate([both_part.astype(BF16), back_part.astype(BF16)], axis=1)
    members = lax.axis_size("row") // 2
    arrived = lax.all_to_all(
        parts.reshape(members, count // members, tall),
        "row",
        0,
        0,
        axis_index_groups=every_other("row"),
        tiled=True,
    )
    summed = jnp.sum(arrived.astype(F32), axis=0)
    gate_val, up_val, back_hidden = (summed[:, k * own : (k + 1) * own] for k in range(3))
    gate_sig = jax.nn.sigmoid(gate_val)
    activation = gate_val * gate_sig
    hidden = (activation * up_val).astype(BF16)
    back_gate = (back_hidden * up_val * gate_sig * (1.0 + gate_val * (1.0 - gate_sig))).astype(BF16)
    back_up = (back_hidden * activation).astype(BF16)
    acts = lax.all_gather(
        jnp.concatenate([back_gate, back_up, hidden], axis=1),
        "row",
        axis=0,
        tiled=True,
        axis_index_groups=every_other("row"),
    )

    def outputs(matrix):
        return [
            row_major(dot(acts[:, wide:], matrix[wide:], NN)),
            row_major(dot(acts[:, :wide], matrix[:wide], NN)),
        ]

    out_pair = jnp.concatenate([value.astype(BF16) for value in outputs(weights_pair)], axis=1)
    out_own, grad_own = outputs(weights)
    near = jnp.concatenate([out_own[half:].astype(BF16), grad_own[half:].astype(BF16)], axis=1)
    pair, far, near, held = lax.optimization_barrier((out_pair[:half], out_pair[half:], near, acts))
    pair = move(pair, True, 0)
    far = move(far, True, -1)
    near = move(near, False, -1)

    def partial_steps(rows):
        return [
            dot(held[:, :wide], rows[:, :features], TN),
            dot(held[:, wide:], rows[:, features:], TN),
        ]

    steps_rest = [value.astype(BF16) for value in partial_steps(rows_pair)]
    steps_rest = move(jnp.concatenate(steps_rest, axis=0), True, 0)
    in_own, last_own = partial_steps(rows_own)
    in_own, last_own = lax.optimization_barrier((in_own, last_own))

    rows = tokens.shape[0]
    padded = round_up(rows + 1, 8) - 1
    sums = scatter_col(spread(core, out_own, grad_own, near, pair, far, rows, padded), rows)
    factor = -step_rate[0]

    def step(mine, rest):
        return (factor * (mine + rest.astype(F32))).astype(BF16)

    sums, step_gate, step_up, step_down = lax.optimization_barrier(
        (
            sums,
            step(in_own[:own], steps_rest[:own]),
            step(in_own[own:], steps_rest[own:wide]),
            step(last_own, steps_rest[wide:]),
        )
    )
    out_rows = (tokens.astype(F32) + sums[:, :features]).astype(BF16)
    grad_in = (cotangent.astype(F32) + sums[:, features:]).astype(BF16)
    return (out_rows, grad_in, step_gate.T, step_up.T, step_down)


def solution(mesh):
    in_specs = (
        P(("sweep", "col"), "row"),
        P("row", "col"),
        P("row", "col"),
        P("col", "row"),
        P(("sweep", "col"), "row"),
        P("sweep"),
    )
    out_specs = (
        P(("sweep", "col"), "row"),
        P(("sweep", "col"), "row"),
        P(("sweep", "row"), "col"),
        P(("sweep", "row"), "col"),
        P(("sweep", "col"), "row"),
    )
    return jax.shard_map(layer, mesh=mesh, in_specs=in_specs, out_specs=out_specs, check_vma=False)
```

```python
import jax
import jax.numpy as jnp
from jax import lax
from jax.experimental import pallas as pl
from jax.experimental.layout import Layout, with_layout_constraint
from jax.experimental.pallas import tpu as pltpu
from jax.sharding import PartitionSpec as P


BF16 = jnp.bfloat16
F32 = jnp.float32
NT = (((1,), (1,)), ((), ()))
NN = (((1,), (0,)), ((), ()))
TN = (((0,), (0,)), ((), ()))


def dot(left, right, dims):
    return lax.dot_general(left, right, dims, preferred_element_type=F32)


def row_major(value):
    return with_layout_constraint(value, Layout(major_to_minor=tuple(range(value.ndim))))


def round_up(value, unit):
    return -(-value // unit) * unit


def every_other(axis):
    size = lax.axis_size(axis)
    return [list(range(first, size, 2)) for first in range(2)]


def move(value, swap, step):
    rows, cols = lax.axis_size("row"), lax.axis_size("col")
    pairs = []
    for row in range(rows):
        for col in range(cols):
            to_row = row ^ 1 if swap else row
            to_col = (col + (step if row % 2 == 0 else -step)) % cols
            pairs.append((row * cols + col, to_row * cols + to_col))
    return lax.ppermute(value, ("row", "col"), pairs)


def gather_col(block):
    return lax.all_gather(block, "col", axis=0, tiled=True, axis_index_groups=every_other("col"))


def spread(core, out_own, grad_own, near, pair, far, rows, padded):
    half, width = near.shape
    features = out_own.shape[1]
    blocks = half // rows

    def kernel(core_ref, out_ref, grad_ref, near_ref, pair_ref, far_ref, sums_ref, same_ref, cross_ref):
        near_rows = near_ref[...].astype(F32)
        same_ref[:, :features] = out_ref[...] + near_rows[:, :features]
        same_ref[:, features:] = grad_ref[...] + near_rows[:, features:]
        cross_ref[...] = pair_ref[...].astype(F32) + far_ref[...].astype(F32)
        for block in range(2 * blocks):
            gap = padded - rows
            sums_ref[block * padded + rows : (block + 1) * padded, :] = jnp.zeros((gap, width), F32)

        def write(low, high):
            for block in range(blocks):
                source = slice(block * rows, (block + 1) * rows)
                for offset, part in ((0, low), (blocks, high)):
                    start = (offset + block) * padded
                    sums_ref[start : start + rows, :] = part[source, :]

        @pl.when(core_ref[0] == 0)
        def _():
            write(same_ref, cross_ref)

        @pl.when(core_ref[0] != 0)
        def _():
            write(cross_ref, same_ref)

    whole = pl.BlockSpec((half, width), lambda _: (0, 0))
    upper = pl.BlockSpec((half, features), lambda _: (0, 0))
    return pl.pallas_call(
        kernel,
        grid=(1,),
        out_shape=jax.ShapeDtypeStruct((2 * blocks * padded, width), F32),
        in_specs=[pl.BlockSpec(memory_space=pltpu.SMEM), upper, upper, whole, whole, whole],
        out_specs=pl.BlockSpec((2 * blocks * padded, width), lambda _: (0, 0)),
        scratch_shapes=[pltpu.VMEM((half, width), F32), pltpu.VMEM((half, width), F32)],
        compiler_params=pltpu.CompilerParams(vmem_limit_bytes=16 << 20),
        name="spread",
    )(core[None], out_own, grad_own, near, pair, far)


def pick(order, wide_part, narrow_part):
    count, wide = wide_part.shape
    width = wide + narrow_part.shape[1]
    chunk = count // order.shape[0]

    def kernel(order_ref, wide_ref, narrow_ref, send_ref, keep_ref):
        for place in range(2):
            rows = slice(place * chunk, (place + 1) * chunk)
            for target, index in ((send_ref, order_ref[place]), (keep_ref, order_ref[place + 2])):
                source = pl.ds(pl.multiple_of(index * chunk, 8), chunk)
                target[rows, :wide] = wide_ref[source, :].astype(target.dtype)
                target[rows, wide:] = narrow_ref[source, :].astype(target.dtype)

    def whole(rows, columns):
        return pl.BlockSpec((rows, columns), lambda _: (0, 0))

    return pl.pallas_call(
        kernel,
        grid=(1,),
        out_shape=(
            jax.ShapeDtypeStruct((2 * chunk, width), BF16),
            jax.ShapeDtypeStruct((2 * chunk, width), F32),
        ),
        in_specs=[
            pl.BlockSpec(memory_space=pltpu.SMEM),
            whole(count, wide),
            whole(count, width - wide),
        ],
        out_specs=(whole(2 * chunk, width), whole(2 * chunk, width)),
        compiler_params=pltpu.CompilerParams(vmem_limit_bytes=16 << 20),
        name="pick",
    )(order, wide_part, narrow_part)


def swap_row(value, stage):
    size = lax.axis_size("row")
    pairs = []
    for row in range(size):
        x, core = row // 2, row % 2
        to_x = x ^ 1 if core == stage else size // 2 - 1 - x
        pairs.append((row, 2 * to_x + core))
    return lax.ppermute(value, "row", pairs)


def sum_row(wide_part, narrow_part):
    row = lax.axis_index("row")
    x, core = row // 2, row % 2
    mirrored = lax.axis_size("row") // 2 - 1 - x
    first = jnp.where(core == 0, x ^ 1, mirrored)
    second = jnp.where(core == 0, mirrored, x ^ 1)
    last = lax.axis_size("row") // 2 - 1 - first
    far = jnp.where(core == 0, last, first ^ 1)
    send, keep = pick(jnp.stack([first, far, x, second]), wide_part, narrow_part)
    chunk = keep.shape[0] // 2
    keep = keep + swap_row(send, 0).astype(F32)
    return keep[:chunk] + swap_row(keep[chunk:].astype(BF16), 1).astype(F32)


def scatter_col(parts, rows):
    summed = lax.psum_scatter(
        parts, "col", scatter_dimension=0, tiled=True, axis_index_groups=every_other("col")
    )
    return lax.optimization_barrier(summed)[:rows]


def layer(tokens, w_gate, w_up, w_down, cotangent, step_rate):
    features = tokens.shape[1]
    own = w_gate.shape[1]
    core = lax.axis_index("row") % 2
    gathered = gather_col(jnp.concatenate([tokens, cotangent], axis=1))
    count = gathered.shape[0]
    half = count // 2
    same = lax.dynamic_slice_in_dim(gathered, core * half, half)
    cross = lax.dynamic_slice_in_dim(gathered, (1 - core) * half, half)
    same, cross, w_gate, w_up, w_down = lax.optimization_barrier(
        (same, cross, w_gate, w_up, w_down)
    )
    weights = jnp.concatenate([w_gate.T, w_up.T, w_down], axis=0)
    rows_own = jnp.concatenate([same, move(same, False, 1)], axis=0)
    rows_pair = jnp.concatenate([move(cross, True, 0), move(cross, True, -1)], axis=0)
    weights_pair = move(weights, True, 0)

    wide = 2 * own
    both_part = dot(rows_own[:, :features], weights[:wide], NT) + dot(
        rows_pair[:, :features], weights_pair[:wide], NT
    )
    back_part = dot(rows_own[:, features:], weights[wide:], NT) + dot(
        rows_pair[:, features:], weights_pair[wide:], NT
    )
    summed = sum_row(both_part, back_part)
    gate_val, up_val, back_hidden = (summed[:, k * own : (k + 1) * own] for k in range(3))
    gate_sig = jax.nn.sigmoid(gate_val)
    activation = gate_val * gate_sig
    hidden = (activation * up_val).astype(BF16)
    back_gate = (back_hidden * up_val * gate_sig * (1.0 + gate_val * (1.0 - gate_sig))).astype(BF16)
    back_up = (back_hidden * activation).astype(BF16)
    acts = lax.all_gather(
        jnp.concatenate([back_gate, back_up, hidden], axis=1),
        "row",
        axis=0,
        tiled=True,
        axis_index_groups=every_other("row"),
    )

    def outputs(matrix):
        return [
            row_major(dot(acts[:, wide:], matrix[wide:], NN)),
            row_major(dot(acts[:, :wide], matrix[:wide], NN)),
        ]

    out_pair = jnp.concatenate([value.astype(BF16) for value in outputs(weights_pair)], axis=1)
    out_own, grad_own = outputs(weights)
    near = jnp.concatenate([out_own[half:].astype(BF16), grad_own[half:].astype(BF16)], axis=1)
    pair, far, near, held = lax.optimization_barrier((out_pair[:half], out_pair[half:], near, acts))
    pair = move(pair, True, 0)
    far = move(far, True, -1)
    near = move(near, False, -1)

    def partial_steps(rows):
        return [
            dot(held[:, :wide], rows[:, :features], TN),
            dot(held[:, wide:], rows[:, features:], TN),
        ]

    steps_rest = [value.astype(BF16) for value in partial_steps(rows_pair)]
    steps_rest = move(jnp.concatenate(steps_rest, axis=0), True, 0)
    in_own, last_own = partial_steps(rows_own)
    in_own, last_own = lax.optimization_barrier((in_own, last_own))

    rows = tokens.shape[0]
    padded = round_up(rows + 1, 8) - 1
    sums = scatter_col(spread(core, out_own, grad_own, near, pair, far, rows, padded), rows)
    factor = -step_rate[0]

    def step(mine, rest):
        return (factor * (mine + rest.astype(F32))).astype(BF16)

    sums, step_gate, step_up, step_down = lax.optimization_barrier(
        (
            sums,
            step(in_own[:own], steps_rest[:own]),
            step(in_own[own:], steps_rest[own:wide]),
            step(last_own, steps_rest[wide:]),
        )
    )
    out_rows = (tokens.astype(F32) + sums[:, :features]).astype(BF16)
    grad_in = (cotangent.astype(F32) + sums[:, features:]).astype(BF16)
    return (out_rows, grad_in, step_gate.T, step_up.T, step_down)


def solution(mesh):
    in_specs = (
        P(("sweep", "col"), "row"),
        P("row", "col"),
        P("row", "col"),
        P("col", "row"),
        P(("sweep", "col"), "row"),
        P("sweep"),
    )
    out_specs = (
        P(("sweep", "col"), "row"),
        P(("sweep", "col"), "row"),
        P(("sweep", "row"), "col"),
        P(("sweep", "row"), "col"),
        P(("sweep", "col"), "row"),
    )
    return jax.shard_map(layer, mesh=mesh, in_specs=in_specs, out_specs=out_specs, check_vma=False)
```

```python
import jax
import jax.numpy as jnp
from jax import lax
from jax.experimental import pallas as pl
from jax.experimental.layout import Layout, with_layout_constraint
from jax.experimental.pallas import tpu as pltpu
from jax.sharding import PartitionSpec as P


BF16 = jnp.bfloat16
F32 = jnp.float32
NT = (((1,), (1,)), ((), ()))
NN = (((1,), (0,)), ((), ()))
TN = (((0,), (0,)), ((), ()))


def dot(left, right, dims):
    return lax.dot_general(left, right, dims, preferred_element_type=F32)


def row_major(value):
    return with_layout_constraint(value, Layout(major_to_minor=tuple(range(value.ndim))))


def round_up(value, unit):
    return -(-value // unit) * unit


def every_other(axis):
    size = lax.axis_size(axis)
    return [list(range(first, size, 2)) for first in range(2)]


def move(value, swap, step):
    rows, cols = lax.axis_size("row"), lax.axis_size("col")
    pairs = []
    for row in range(rows):
        for col in range(cols):
            to_row = row ^ 1 if swap else row
            to_col = (col + (step if row % 2 == 0 else -step)) % cols
            pairs.append((row * cols + col, to_row * cols + to_col))
    return lax.ppermute(value, ("row", "col"), pairs)


def gather_col(block):
    return lax.all_gather(block, "col", axis=0, tiled=True, axis_index_groups=every_other("col"))


def row_parts(rows_own, rows_pair, weights, weights_pair):
    count, width = rows_own.shape
    features = width // 2
    tall = weights.shape[0]
    wide = tall // 3 * 2
    step = 256
    edges = [*range(0, wide, step), *range(wide, tall, step), tall]

    def kernel(own_ref, pair_ref, weights_ref, pair_weights_ref, parts_ref):
        for low, high in zip(edges, edges[1:]):
            columns = slice(0, features) if low < wide else slice(features, width)
            total = dot(own_ref[:, columns], weights_ref[low:high, :], NT)
            total += dot(pair_ref[:, columns], pair_weights_ref[low:high, :], NT)
            parts_ref[:, low:high] = total.astype(BF16)

    def whole(shape):
        return pl.BlockSpec(shape, lambda _: (0, 0))

    return pl.pallas_call(
        kernel,
        grid=(1,),
        out_shape=jax.ShapeDtypeStruct((count, tall), BF16),
        in_specs=[whole(v.shape) for v in (rows_own, rows_pair, weights, weights_pair)],
        out_specs=whole((count, tall)),
        compiler_params=pltpu.CompilerParams(vmem_limit_bytes=24 << 20),
        name="row_parts",
    )(rows_own, rows_pair, weights, weights_pair)


def spread(core, out_own, grad_own, near, pair, far, rows, padded):
    half, width = near.shape
    features = out_own.shape[1]
    blocks = half // rows

    def kernel(core_ref, out_ref, grad_ref, near_ref, pair_ref, far_ref, sums_ref, same_ref, cross_ref):
        near_rows = near_ref[...].astype(F32)
        same_ref[:, :features] = out_ref[...] + near_rows[:, :features]
        same_ref[:, features:] = grad_ref[...] + near_rows[:, features:]
        cross_ref[...] = pair_ref[...].astype(F32) + far_ref[...].astype(F32)
        for block in range(2 * blocks):
            gap = padded - rows
            sums_ref[block * padded + rows : (block + 1) * padded, :] = jnp.zeros((gap, width), F32)

        def write(low, high):
            for block in range(blocks):
                source = slice(block * rows, (block + 1) * rows)
                for offset, part in ((0, low), (blocks, high)):
                    start = (offset + block) * padded
                    sums_ref[start : start + rows, :] = part[source, :]

        @pl.when(core_ref[0] == 0)
        def _():
            write(same_ref, cross_ref)

        @pl.when(core_ref[0] != 0)
        def _():
            write(cross_ref, same_ref)

    whole = pl.BlockSpec((half, width), lambda _: (0, 0))
    upper = pl.BlockSpec((half, features), lambda _: (0, 0))
    return pl.pallas_call(
        kernel,
        grid=(1,),
        out_shape=jax.ShapeDtypeStruct((2 * blocks * padded, width), F32),
        in_specs=[pl.BlockSpec(memory_space=pltpu.SMEM), upper, upper, whole, whole, whole],
        out_specs=pl.BlockSpec((2 * blocks * padded, width), lambda _: (0, 0)),
        scratch_shapes=[pltpu.VMEM((half, width), F32), pltpu.VMEM((half, width), F32)],
        compiler_params=pltpu.CompilerParams(vmem_limit_bytes=16 << 20),
        name="spread",
    )(core[None], out_own, grad_own, near, pair, far)


def scatter_col(parts, rows):
    summed = lax.psum_scatter(
        parts, "col", scatter_dimension=0, tiled=True, axis_index_groups=every_other("col")
    )
    return lax.optimization_barrier(summed)[:rows]


def layer(tokens, w_gate, w_up, w_down, cotangent, step_rate):
    features = tokens.shape[1]
    own = w_gate.shape[1]
    core = lax.axis_index("row") % 2
    gathered = gather_col(jnp.concatenate([tokens, cotangent], axis=1))
    count = gathered.shape[0]
    half = count // 2
    same = lax.dynamic_slice_in_dim(gathered, core * half, half)
    cross = lax.dynamic_slice_in_dim(gathered, (1 - core) * half, half)
    same, cross, w_gate, w_up, w_down = lax.optimization_barrier(
        (same, cross, w_gate, w_up, w_down)
    )
    weights = jnp.concatenate([w_gate.T, w_up.T, w_down], axis=0)
    rows_own = jnp.concatenate([same, move(same, False, 1)], axis=0)
    rows_pair = jnp.concatenate([move(cross, True, 0), move(cross, True, -1)], axis=0)
    weights_pair = move(weights, True, 0)

    wide = 2 * own
    tall = 3 * own
    parts = row_parts(rows_own, rows_pair, weights, weights_pair)
    members = lax.axis_size("row") // 2
    arrived = lax.all_to_all(
        parts.reshape(members, count // members, tall),
        "row",
        0,
        0,
        axis_index_groups=every_other("row"),
        tiled=True,
    )
    summed = jnp.sum(arrived.astype(F32), axis=0)
    gate_val, up_val, back_hidden = (summed[:, k * own : (k + 1) * own] for k in range(3))
    gate_sig = jax.nn.sigmoid(gate_val)
    activation = gate_val * gate_sig
    hidden = (activation * up_val).astype(BF16)
    back_gate = (back_hidden * up_val * gate_sig * (1.0 + gate_val * (1.0 - gate_sig))).astype(BF16)
    back_up = (back_hidden * activation).astype(BF16)
    acts = lax.all_gather(
        jnp.concatenate([back_gate, back_up, hidden], axis=1),
        "row",
        axis=0,
        tiled=True,
        axis_index_groups=every_other("row"),
    )

    def outputs(matrix):
        return [
            row_major(dot(acts[:, wide:], matrix[wide:], NN)),
            row_major(dot(acts[:, :wide], matrix[:wide], NN)),
        ]

    out_pair = jnp.concatenate([value.astype(BF16) for value in outputs(weights_pair)], axis=1)
    out_own, grad_own = outputs(weights)
    near = jnp.concatenate([out_own[half:].astype(BF16), grad_own[half:].astype(BF16)], axis=1)
    pair, far, near, held = lax.optimization_barrier((out_pair[:half], out_pair[half:], near, acts))
    pair = move(pair, True, 0)
    far = move(far, True, -1)
    near = move(near, False, -1)

    def partial_steps(rows):
        return [
            dot(held[:, :wide], rows[:, :features], TN),
            dot(held[:, wide:], rows[:, features:], TN),
        ]

    steps_rest = [value.astype(BF16) for value in partial_steps(rows_pair)]
    steps_rest = move(jnp.concatenate(steps_rest, axis=0), True, 0)
    in_own, last_own = partial_steps(rows_own)
    in_own, last_own = lax.optimization_barrier((in_own, last_own))

    rows = tokens.shape[0]
    padded = round_up(rows + 1, 8) - 1
    sums = scatter_col(spread(core, out_own, grad_own, near, pair, far, rows, padded), rows)
    factor = -step_rate[0]

    def step(mine, rest):
        return (factor * (mine + rest.astype(F32))).astype(BF16)

    sums, step_gate, step_up, step_down = lax.optimization_barrier(
        (
            sums,
            step(in_own[:own], steps_rest[:own]),
            step(in_own[own:], steps_rest[own:wide]),
            step(last_own, steps_rest[wide:]),
        )
    )
    out_rows = (tokens.astype(F32) + sums[:, :features]).astype(BF16)
    grad_in = (cotangent.astype(F32) + sums[:, features:]).astype(BF16)
    return (out_rows, grad_in, step_gate.T, step_up.T, step_down)


def solution(mesh):
    in_specs = (
        P(("sweep", "col"), "row"),
        P("row", "col"),
        P("row", "col"),
        P("col", "row"),
        P(("sweep", "col"), "row"),
        P("sweep"),
    )
    out_specs = (
        P(("sweep", "col"), "row"),
        P(("sweep", "col"), "row"),
        P(("sweep", "row"), "col"),
        P(("sweep", "row"), "col"),
        P(("sweep", "col"), "row"),
    )
    return jax.shard_map(layer, mesh=mesh, in_specs=in_specs, out_specs=out_specs, check_vma=False)
```
